64 devices in a mesh: dp: 4 (over x, y), sp: 16 (over z, core).
Axes of the slice: x: 2, y: 2, z: 8, core: 2. Of those that a mesh axis runs over, the one named last changes fastest.
The devices are a block of a 4x4x8 slice.
Arguments:
- x: bfloat16 [32768, 2048], P(('dp', 'sp')), parts along dimension 0
- gain: bfloat16 [2048], replicated
- wq: bfloat16 [2048, 2048], P('sp')
- wk: bfloat16 [2048, 256], P('sp')
- wv: bfloat16 [2048, 256], P('sp')
- wo: bfloat16 [2048, 2048], P('sp')
Outputs:
- output: bfloat16 [32768, 2048], P(('dp', 'sp')), parts along dimension 0
There are 4 independent parts. The reference program is written for one: setup_inputs(seed, part) draws one part's arguments, and reference() takes and returns one part's arrays. A program takes and returns all parts, laid end to end along the dimension named above; an argument that names none is the same for every part.
All inputs are finite; a program needn't handle non-finite values.
Results may differ from the reference program's by a relative error of at most 0.012.
Values are sent between devices in bfloat16 or wider.
A program may use at most 768 MiB of HBM per device.

```python
import jax
import jax.numpy as jnp
from jax import lax

ROWS = 8192
D = 2048
HEADS = 8
KV_HEADS = 1
HEAD = 256
THETA = 10000


def setup_inputs(seed: int = 0, part: int = 0) -> dict:
    kx, kn, kq, kk, kv, ko = jax.random.split(jax.random.key(seed), 6)

    def weights(key, rows, columns):
        return jax.random.normal(key, (rows, columns), jnp.float32) * rows**-0.5

    drawn = {
        "x": jax.random.normal(jax.random.fold_in(kx, part), (ROWS, D), jnp.float32),
        "gain": 1 + 0.1 * jax.random.normal(kn, (D,), jnp.float32),
        "wq": 2 * weights(kq, D, HEADS * HEAD),
        "wk": 2 * weights(kk, D, KV_HEADS * HEAD),
        "wv": 4 * weights(kv, D, KV_HEADS * HEAD),
        "wo": weights(ko, HEADS * HEAD, D),
    }
    return {k: v.astype(jnp.bfloat16) for k, v in drawn.items()}


def normed(x, gain):
    wide = x.astype(jnp.float32)
    scale = lax.rsqrt(jnp.mean(wide * wide, -1, keepdims=True) + 1e-6)
    return (wide * scale * gain.astype(jnp.float32)).astype(jnp.bfloat16)


def turned(t, place, theta):
    half = t.shape[-1] // 2
    angle = place.astype(jnp.float32)[:, None] * theta ** (-jnp.arange(half, dtype=jnp.float32) / half)
    cos, sin = jnp.cos(angle)[:, None], jnp.sin(angle)[:, None]
    a, b = t[..., :half].astype(jnp.float32), t[..., half:].astype(jnp.float32)
    return jnp.concatenate([a * cos - b * sin, b * cos + a * sin], -1).astype(jnp.bfloat16)


def matmul(a, w):
    return jnp.dot(a, w, preferred_element_type=jnp.float32).astype(jnp.bfloat16)


def einsum(form, a, b):
    return jnp.einsum(form, a.astype(jnp.float32), b.astype(jnp.float32))


def attention(q, k, v):
    scores = einsum("tgsd,ugd->gstu", q, k) * q.shape[-1] ** -0.5
    token = jnp.arange(q.shape[0])
    scores = jnp.where(token[:, None] >= token, scores, -jnp.inf)
    weights = jax.nn.softmax(scores, -1).astype(jnp.bfloat16)
    return einsum("gstu,ugd->tgsd", weights, v).astype(jnp.bfloat16)


def reference(x, gain, wq, wk, wv, wo):
    a, place = normed(x, gain), jnp.arange(ROWS)
    q = turned(matmul(a, wq).reshape(ROWS, HEADS, HEAD), place, THETA).reshape(ROWS, KV_HEADS, -1, HEAD)
    k = turned(matmul(a, wk).reshape(ROWS, KV_HEADS, HEAD), place, THETA)
    v = matmul(a, wv).reshape(ROWS, KV_HEADS, HEAD)
    seen = attention(q, k, v).reshape(ROWS, HEADS * HEAD)
    return (x.astype(jnp.float32) + jnp.dot(seen, wo, preferred_element_type=jnp.float32)).astype(jnp.bfloat16)
```

```python
import functools
import math

import jax
import jax.numpy as jnp
from jax import lax
from jax.experimental import pallas as pl
from jax.experimental.pallas import tpu as pltpu
from jax.sharding import PartitionSpec as P

HEAD = 256
THETA = 10000
NEG = -1e30
HIDDEN = 2 * NEG
LOG2E = 1.4426950408889634
MESH = pl.DeviceIdType.MESH
VMEM_LIMIT = 67_043_328
F32, BF16 = jnp.float32, jnp.bfloat16
PIECES = ((0, 0), (1, 1), (0, 1), (1, 0))


def _dot(a, b):
    return lax.dot_general(a, b, (((1,), (0,)), ((), ())), preferred_element_type=F32)


def _kernel(side, x_hbm, gain_ref, freq_ref, wq_hbm, wk_hbm, wv_hbm, wo_hbm, y_hbm, w1, w2, kall, vall, xs, a, acc, qt, mix, top, seen, cos_s, sin_s,
            local, z1, xy1, d1, s1, z2, xy2, d2, s2, zk, dk, sk, sd, out_sem):
    own, depth = xs.shape
    nd = kall.shape[0]
    ring = nd // 2
    far = ring // 2
    heads = qt.shape[0]
    rows = depth // nd
    piece = rows // 4

    me, dp = lax.axis_index("sp"), lax.axis_index("dp")
    z, lane = lax.div(me, 2), lax.rem(me, 2)
    gx, gy = lax.div(dp, side), lax.rem(dp, side)
    ox, oy = 1 - 2 * lax.rem(gx, 2), 1 - 2 * lax.rem(gy, 2)
    par = lax.rem(gx + gy, 2)
    around = ((dp, 2 * lax.rem(z + 1, ring) + lane), (dp, 2 * lax.rem(z + ring - 1, ring) + lane))
    partner = ((dp + ox * side, me), (dp + oy, me))
    mate = (dp, 2 * z + 1 - lane)

    def hops(d, e):
        return far if d == e else far - 1

    def chip(d, t):
        return lax.rem(z + ring - t, ring) if d == 0 else lax.rem(z + t, ring)

    def remote(ref, send, recv, to):
        return pltpu.make_async_remote_copy(src_ref=ref, dst_ref=ref, send_sem=send, recv_sem=recv, device_id=to, device_id_type=MESH)

    def arrive(ref, recv, send):
        remote(ref, send, recv, mate).wait_recv()

    def part(w, ch, half, e):
        return w.at[pl.ds(pl.multiple_of(ch * 2 * rows + lane * rows + half * 2 * piece + e * piece, piece), piece), :]

    def shard(w, ch, ln):
        return w.at[pl.ds(pl.multiple_of(ch * 2 * rows + ln * rows, rows), rows), :]

    def w_start(w, zs, ds, ss):
        for d, e in PIECES:
            remote(part(w, z, par, e), ss, zs.at[d, e, 1], around[d]).start()
        remote(shard(w, z, lane), ss, ds.at[0, 0], mate).start()

    def w_ring(w, zs, xys, ss, t):
        for d, e in PIECES:
            def go(d=d, e=e):
                ref = part(w, chip(d, t), par, e)
                arrive(ref, zs.at[d, e, t], ss)

                @pl.when(t < hops(d, e))
                def _():
                    remote(ref, ss, zs.at[d, e, t + 1], around[d]).start()

                remote(ref, ss, xys.at[d, e, t], partner[e]).start()

            pl.when(t <= hops(d, e))(go)

    def w_cross(w, xys, ds, ss, t):
        for d, e in PIECES:
            @pl.when(t <= hops(d, e))
            def _(d=d, e=e):
                arrive(part(w, chip(d, t), 1 - par, e), xys.at[d, e, t], ss)
        remote(shard(w, chip(0, t), lane), ss, ds.at[0, t], mate).start()

        @pl.when(t < far)
        def _():
            remote(shard(w, chip(1, t), lane), ss, ds.at[1, t], mate).start()

    def w_mate(w, ds, ss, t):
        arrive(shard(w, chip(0, t), 1 - lane), ds.at[0, t], ss)

        @pl.when((t > 0) & (t < far))
        def _():
            arrive(shard(w, chip(1, t), 1 - lane), ds.at[1, t], ss)

    def w_drain(w, ss):
        total = 4 * (2 * far - 1) * piece + nd * rows // 2
        remote(w.at[pl.ds(0, total), :], ss, ss, mate).wait_send()

    barrier = pltpu.get_barrier_semaphore()
    for to in (*around, *partner, mate):
        pl.semaphore_signal(barrier, inc=1, device_id=to, device_id_type=MESH)
    mine = pl.ds(pl.multiple_of(me * rows, rows), rows)
    loads = [
        pltpu.make_async_copy(wk_hbm, w1.at[mine, pl.ds(0, HEAD)], local.at[0]),
        pltpu.make_async_copy(wv_hbm, w1.at[mine, pl.ds(HEAD, HEAD)], local.at[1]),
        pltpu.make_async_copy(wq_hbm, w1.at[mine, pl.ds(2 * HEAD, heads * HEAD)], local.at[2]),
        pltpu.make_async_copy(x_hbm, xs, local.at[3]),
        pltpu.make_async_copy(wo_hbm, w2.at[mine, :], local.at[4]),
    ]
    for load in loads:
        load.start()
    for load in loads[:3]:
        load.wait()
    pl.semaphore_wait(barrier, 5)
    w_start(w1, z1, d1, s1)
    loads[3].wait()

    tile = 64

    def norm(i, _):
        at = pl.ds(pl.multiple_of(i * tile, tile), tile)
        wide = xs[at, :].astype(F32)
        scale = lax.rsqrt(jnp.mean(wide * wide, -1, keepdims=True) + 1e-6)
        a[at, :] = (wide * scale * gain_ref[...].astype(F32)).astype(BF16)
        place = (lax.broadcasted_iota(jnp.int32, (tile, HEAD // 2), 0) + (me * own + i * tile)).astype(F32)
        angle = place * freq_ref[...]
        cos_s[at, :] = jnp.cos(angle)
        sin_s[at, :] = jnp.sin(angle)

    lax.fori_loop(0, own // tile, norm, None)
    loads[4].wait()

    wide = 512

    def project(chips, first, lo, hi):
        def tiles(n, _):
            at = pl.ds(pl.multiple_of(n * wide, wide), wide)
            total = None
            for ch in chips:
                deep = pl.ds(pl.multiple_of(ch * 2 * rows, 2 * rows), 2 * rows)
                term = _dot(a[:, deep], w1[deep, at])
                total = term if total is None else total + term
            acc[:, at] = total if first else acc[:, at] + total

        lax.fori_loop(lo, hi, tiles, None)

    count = acc.shape[1] // wide
    for t in range(1, far + 1):
        w_ring(w1, z1, xy1, s1, t)
        if t == far - 1:
            w_start(w2, z2, d2, s2)
        if t > 1:
            w_cross(w1, xy1, d1, s1, t - 1)
        if t == 1:
            w_mate(w1, d1, s1, 0)
            project([z], True, 0, count)
        if t > 2:
            w_mate(w1, d1, s1, t - 2)
            project([chip(0, t - 2), chip(1, t - 2)], False, 0, count)
    w_mate(w1, d1, s1, far - 1)
    project([chip(0, far - 1), chip(1, far - 1)], False, 0, count)
    w_ring(w2, z2, xy2, s2, 1)
    w_cross(w1, xy1, d1, s1, far)
    w_mate(w1, d1, s1, far)
    project([chip(0, far)], False, 0, 1)

    def turned(t):
        t = t.astype(BF16)
        half = HEAD // 2
        lo, hi = t[:, :half].astype(F32), t[:, half:].astype(F32)
        c, s = cos_s[...], sin_s[...]
        return jnp.concatenate([lo * c - hi * s, hi * c + lo * s], -1).astype(BF16)

    kall[me] = turned(acc[:, :HEAD])
    vall[me] = acc[:, HEAD : 2 * HEAD].astype(BF16).T
    project([chip(0, far)], False, 1, count)

    bufs = (kall, vall)

    def block(e, ch, ln):
        return bufs[e].at[2 * ch + ln]

    for d, e in PIECES:
        remote(block(e, z, lane), sk, zk.at[d, e, 1], around[d]).start()
    for e in (0, 1):
        remote(block(e, z, lane), sd, dk.at[0, e, 0], mate).start()

    def turn_head(h, _):
        at = pl.ds(pl.multiple_of((2 + h) * HEAD, HEAD), HEAD)
        qt[h] = turned(acc[:, at]).T

    lax.fori_loop(0, heads, turn_head, None)

    def kv_ring(t):
        for d, e in PIECES:
            def go(d=d, e=e):
                ref = block(e, chip(d, t), lane)
                arrive(ref, zk.at[d, e, t], sk)

                @pl.when(t < hops(d, e))
                def _():
                    remote(ref, sk, zk.at[d, e, t + 1], around[d]).start()

                remote(ref, sd, dk.at[d, e, t], mate).start()

            pl.when((t > 0) & (t <= hops(d, e)))(go)

    def kv_mate(t):
        for d, e in PIECES:
            cond = (t <= hops(d, e)) if d == 0 else (t > 0) & (t <= hops(d, e))

            @pl.when(cond)
            def _(d=d, e=e):
                arrive(block(e, chip(d, t), 1 - lane), dk.at[d, e, t], sk)

    scale = HEAD**-0.5 * LOG2E
    top[...] = jnp.full(top.shape, NEG, F32)
    mix[...] = jnp.zeros(mix.shape, F32)

    def attend(b, masked):
        keys = kall[b]
        scores = [_dot(keys, qt[h]) for h in range(heads)]
        if masked:
            ok = lax.broadcasted_iota(jnp.int32, (own, own), 1) >= lax.broadcasted_iota(jnp.int32, (own, own), 0)
        weights, keeps = [], []
        for h, s in enumerate(scores):
            if masked:
                s = jnp.where(ok, s, HIDDEN)
            old = top[h : h + 1, :]
            new = jnp.maximum(old, s.max(axis=0, keepdims=True))
            top[h : h + 1, :] = new
            weights.append(jnp.exp2((s - new) * scale).astype(BF16))
            keeps.append(jnp.exp2((old - new) * scale))
        values = jnp.concatenate([vall[b], jnp.ones((8, own), BF16)], axis=0)
        for h in range(heads):
            mix[h] = mix[h] * keeps[h] + _dot(values, weights[h])

    attend(me, True)

    def ring_step(t, _):
        kv_ring(t)

        def quarter(i, _):
            @pl.when(i == 2)
            def _():
                kv_mate(t)

                @pl.when((t > 0) & (t < far))
                def _():
                    w_ring(w2, z2, xy2, s2, t + 1)

                @pl.when(t > 0)
                def _():
                    w_cross(w2, xy2, d2, s2, t)

            d, other = lax.rem(i, 2), lax.div(i, 2)
            ln = lane + other * (1 - 2 * lane)
            ch = z - t + d * (2 * t - ring)
            near = (d == 0) & (other == 1) & (lane == 1)
            seen_chip = (ch >= 0) & ((d == 0) | (t < far))

            @pl.when(((t == 0) & near) | ((t > 0) & seen_chip))
            def _():
                attend(2 * ch + ln, False)

        lax.fori_loop(0, 4, quarter, None)

    lax.fori_loop(0, far + 1, ring_step, None)

    for h in range(heads):
        total = mix[h, HEAD : HEAD + 1, :]
        seen[:, h * HEAD : (h + 1) * HEAD] = (mix[h, :HEAD, :] * (1 / total)).T.astype(BF16)
    for t in range(far + 1):
        w_mate(w2, d2, s2, t)
    n_out = depth // wide

    def out_copy(n):
        at = pl.ds(pl.multiple_of(n * wide, wide), wide)
        return pltpu.make_async_copy(a.at[:, at], y_hbm.at[:, at], out_sem.at[n])

    def finish(n, _):
        at = pl.ds(pl.multiple_of(n * wide, wide), wide)
        a[:, at] = (xs[:, at].astype(F32) + _dot(seen[...], w2[:, at])).astype(BF16)
        out_copy(n).start()

    lax.fori_loop(0, n_out, finish, None)
    w_drain(w1, s1)
    w_drain(w2, s2)
    remote(kall.at[pl.ds(0, 2 * (2 * far - 1))], sk, sk, mate).wait_send()
    remote(kall, sd, sd, mate).wait_send()
    for n in range(n_out):
        out_copy(n).wait()


def solution(mesh):
    side = math.isqrt(mesh.shape["dp"])
    nd = mesh.shape["sp"]
    far = nd // 4

    def step(x, gain, wq, wk, wv, wo):
        own, depth = x.shape
        heads = wq.shape[1] // HEAD
        freq = (THETA ** (-jnp.arange(HEAD // 2, dtype=F32) / (HEAD // 2)))[None]
        anywhere = pl.BlockSpec(memory_space=pl.ANY)
        vmem = pl.BlockSpec(memory_space=pltpu.VMEM)
        dma = pltpu.SemaphoreType.DMA
        width = wq.shape[1] + wk.shape[1] + wv.shape[1]
        flops = 2 * own * depth * width + 2 * own * heads * HEAD * depth + 4 * own * own * nd * heads * HEAD // 2
        return pl.pallas_call(
            functools.partial(_kernel, side),
            out_shape=jax.ShapeDtypeStruct(x.shape, x.dtype),
            in_specs=[anywhere, vmem, vmem, anywhere, anywhere, anywhere, anywhere],
            out_specs=anywhere,
            scratch_shapes=[
                pltpu.VMEM((depth, width), BF16),
                pltpu.VMEM((heads * HEAD, depth), BF16),
                pltpu.VMEM((nd, own, HEAD), BF16),
                pltpu.VMEM((nd, HEAD, own), BF16),
                pltpu.VMEM((own, depth), BF16),
                pltpu.VMEM((own, depth), BF16),
                pltpu.VMEM((own, width), F32),
                pltpu.VMEM((heads, HEAD, own), BF16),
                pltpu.VMEM((heads, HEAD + 8, own), F32),
                pltpu.VMEM((heads, own), F32),
                pltpu.VMEM((own, heads * HEAD), BF16),
                pltpu.VMEM((own, HEAD // 2), F32),
                pltpu.VMEM((own, HEAD // 2), F32),
                dma((5,)),
                dma((2, 2, far + 1)), dma((2, 2, far + 1)), dma((2, far + 1)), dma,
                dma((2, 2, far + 1)), dma((2, 2, far + 1)), dma((2, far + 1)), dma,
                dma((2, 2, far + 1)), dma((2, 2, far + 1)), dma, dma,
                dma((depth // 512,)),
            ],
            compiler_params=pltpu.CompilerParams(collective_id=0, has_side_effects=True, vmem_limit_bytes=VMEM_LIMIT),
            cost_estimate=pl.CostEstimate(flops=flops, bytes_accessed=4 * x.size * 2, transcendentals=own * own * nd * heads // 2),
        )(x, gain[None], freq, wq, wk, wv, wo)

    tokens, whole = P(("dp", "sp"), None), P("sp", None)
    return jax.shard_map(
        step,
        mesh=mesh,
        in_specs=(tokens, P(None), whole, whole, whole, whole),
        out_specs=tokens,
        check_vma=False,
    )
```

```python
import functools
import math

import jax
import jax.numpy as jnp
from jax import lax
from jax.experimental import pallas as pl
from jax.experimental.pallas import tpu as pltpu
from jax.sharding import PartitionSpec as P

HEAD = 256
THETA = 10000
NEG = -1e30
HIDDEN = 2 * NEG
LOG2E = 1.4426950408889634
MESH = pl.DeviceIdType.MESH
VMEM_LIMIT = 67_043_328
F32, BF16 = jnp.float32, jnp.bfloat16
PIECES = ((0, 0), (1, 1), (0, 1), (1, 0))


def _dot(a, b):
    return lax.dot_general(a, b, (((1,), (0,)), ((), ())), preferred_element_type=F32)


def _kernel(side, x_hbm, gain_ref, wq_hbm, wk_hbm, wv_hbm, wo_hbm, y_hbm, wkv, wq, wo, kall, vall, xs, a, acc, qt, mix, top, seen, cos_s, sin_s,
            local, zkv, xkv, dkv, skv, zq, xq, dq, sq, zo, xo, go, do, so, zk, dk, sk, sd, out_sem):
    own, depth = xs.shape
    nd = kall.shape[0]
    ring = nd // 2
    far = ring // 2
    heads = qt.shape[0]
    rows = depth // nd

    me, dp = lax.axis_index("sp"), lax.axis_index("dp")
    z, lane = lax.div(me, 2), lax.rem(me, 2)
    gx, gy = lax.div(dp, side), lax.rem(dp, side)
    px, py = lax.rem(gx, 2), lax.rem(gy, 2)
    par = lax.rem(px + py, 2)
    around = ((dp, 2 * lax.rem(z + 1, ring) + lane), (dp, 2 * lax.rem(z + ring - 1, ring) + lane))
    partner = ((dp + (1 - 2 * px) * side, me), (dp + 1 - 2 * py, me))
    mate = (dp, 2 * z + 1 - lane)

    def hops(d, e):
        return far if d == e else far - 1

    def chip(d, t):
        return lax.rem(z + ring - t, ring) if d == 0 else lax.rem(z + t, ring)

    def remote(ref, send, recv, to):
        return pltpu.make_async_remote_copy(src_ref=ref, dst_ref=ref, send_sem=send, recv_sem=recv, device_id=to, device_id_type=MESH)

    def arrive(ref, recv):
        remote(ref, recv, recv, mate).wait_recv()

    def cut(w, ch, ln, at, size):
        return w.at[pl.ds(pl.multiple_of((2 * ch + ln) * rows + at, size), size), :]

    class Halves:
        def __init__(self, w, zs, xs_, ds, ss):
            self.w, self.zs, self.xs, self.ds, self.ss = w, zs, xs_, ds, ss

        def part(self, ch, half, e):
            return cut(self.w, ch, lane, half * (rows // 2) + e * (rows // 4), rows // 4)

        def half(self, ch, ln, half):
            return cut(self.w, ch, ln, half * (rows // 2), rows // 2)

        def start(self, pieces):
            for d, e in pieces:
                remote(self.part(z, par, e), self.ss, self.zs.at[d, e, 1], around[d]).start()

        def start_mate(self):
            remote(cut(self.w, z, lane, 0, rows), self.ss, self.ds.at[0, 0, 0], mate).start()

        def ring(self, pieces, t):
            for d, e in pieces:
                if t <= hops(d, e):
                    ref = self.part(chip(d, t), par, e)
                    arrive(ref, self.zs.at[d, e, t])
                    if t < hops(d, e):
                        remote(ref, self.ss, self.zs.at[d, e, t + 1], around[d]).start()
                    remote(ref, self.ss, self.xs.at[d, e, t], partner[e]).start()

        def mate_ring(self, t):
            for d in (0, 1) if t < far else (0,):
                remote(self.half(chip(d, t), lane, par), self.ss, self.ds.at[0, d, t], mate).start()

        def cross(self, t):
            for d, e in PIECES:
                if t <= hops(d, e):
                    arrive(self.part(chip(d, t), 1 - par, e), self.xs.at[d, e, t])
            for d in (0, 1) if t < far else (0,):
                remote(self.half(chip(d, t), lane, 1 - par), self.ss, self.ds.at[1, d, t], mate).start()

        def mate(self, t):
            if t == 0:
                arrive(cut(self.w, z, 1 - lane, 0, rows), self.ds.at[0, 0, 0])
                return
            for d in (0, 1) if t < far else (0,):
                arrive(self.half(chip(d, t), 1 - lane, par), self.ds.at[0, d, t])
                arrive(self.half(chip(d, t), 1 - lane, 1 - par), self.ds.at[1, d, t])

    def drain(w, ss):
        total = (2 * far - 1) * rows + nd * rows // 2
        remote(w.at[pl.ds(0, total), :], ss, ss, mate).wait_send()

    kvw, qw = Halves(wkv, zkv, xkv, dkv, skv), Halves(wq, zq, xq, dq, sq)
    early, late = PIECES[:2], PIECES[2:]

    quarter_of = (2 * px + py, 2 * (1 - px) + py, 2 * px + 1 - py, 2 * (1 - px) + 1 - py)

    def out_part(ch, which, e):
        return cut(wo, ch, lane, quarter_of[which] * (rows // 4) + e * (rows // 8), rows // 8)

    def wo_start():
        for d, e in PIECES:
            remote(out_part(z, 0, e), so, zo.at[d, e, 1], around[d]).start()

    def wo_ring(t):
        for d, e in PIECES:
            @pl.when(t <= hops(d, e))
            def _(d=d, e=e):
                ref = out_part(chip(d, t), 0, e)
                arrive(ref, zo.at[d, e, t])

                @pl.when(t < hops(d, e))
                def _():
                    remote(ref, so, zo.at[d, e, t + 1], around[d]).start()

                for p in (0, 1):
                    remote(ref, so, xo.at[p, d, e, t], partner[p]).start()

    def wo_cross(t):
        for d, e in PIECES:
            @pl.when(t <= hops(d, e))
            def _(d=d, e=e):
                for p in (0, 1):
                    ref = out_part(chip(d, t), 1 + p, e)
                    arrive(ref, xo.at[p, d, e, t])
                    if p == e:
                        remote(ref, so, go.at[d, e, t], partner[1 - p]).start()

    def wo_fourth(t):
        for d, e in PIECES:
            @pl.when(t <= hops(d, e))
            def _(d=d, e=e):
                arrive(out_part(chip(d, t), 3, e), go.at[d, e, t])
        remote(cut(wo, chip(0, t), lane, 0, rows), so, do.at[0, t], mate).start()

        @pl.when(t < far)
        def _():
            remote(cut(wo, chip(1, t), lane, 0, rows), so, do.at[1, t], mate).start()

    barrier = pltpu.get_barrier_semaphore()
    for to in (*around, *partner, mate):
        pl.semaphore_signal(barrier, inc=1, device_id=to, device_id_type=MESH)
    mine = pl.ds(pl.multiple_of(me * rows, rows), rows)
    loads = [
        pltpu.make_async_copy(wk_hbm, wkv.at[mine, pl.ds(0, HEAD)], local.at[0]),
        pltpu.make_async_copy(wv_hbm, wkv.at[mine, pl.ds(HEAD, HEAD)], local.at[1]),
        pltpu.make_async_copy(wq_hbm, wq.at[mine, :], local.at[2]),
        pltpu.make_async_copy(x_hbm, xs, local.at[3]),
        pltpu.make_async_copy(wo_hbm, wo.at[mine, :], local.at[4]),
    ]
    for load in loads:
        load.start()
    loads[0].wait()
    loads[1].wait()
    pl.semaphore_wait(barrier, 5)
    kvw.start(PIECES)
    kvw.start_mate()
    loads[2].wait()
    qw.start(early)
    qw.start_mate()
    loads[3].wait()

    tile = 64
    freq = jnp.exp(lax.broadcasted_iota(jnp.int32, (1, HEAD // 2), 1).astype(F32) * (-math.log(THETA) / (HEAD // 2)))

    def norm(i, _):
        at = pl.ds(pl.multiple_of(i * tile, tile), tile)
        wide = xs[at, :].astype(F32)
        scale = lax.rsqrt(jnp.mean(wide * wide, -1, keepdims=True) + 1e-6)
        a[at, :] = (wide * scale * gain_ref[...].reshape(1, depth).astype(F32)).astype(BF16)

    def angles(i, _):
        at = pl.ds(pl.multiple_of(i * tile, tile), tile)
        place = (lax.broadcasted_iota(jnp.int32, (tile, HEAD // 2), 0) + (me * own + i * tile)).astype(F32)
        angle = place * freq
        cos_s[at, :] = jnp.cos(angle)
        sin_s[at, :] = jnp.sin(angle)

    lax.fori_loop(0, own // tile, norm, None)
    kvw.ring(PIECES, 1)
    qw.start(late)
    kvw.mate_ring(1)
    lax.fori_loop(0, own // tile, angles, None)
    kvw.ring(PIECES, 2)
    kvw.mate_ring(2)
    qw.ring(early, 1)
    loads[4].wait()
    kvw.cross(1)
    kvw.ring(PIECES, 3)
    kvw.mate_ring(3)
    qw.ring(late, 1)

    wide = 512

    def project(chips, first):
        def tiles(n, _):
            at = pl.ds(pl.multiple_of(n * wide, wide), wide)
            total = None
            for ch in chips:
                deep = pl.ds(pl.multiple_of(ch * 2 * rows, 2 * rows), 2 * rows)
                term = _dot(a[:, deep], wq[deep, at])
                total = term if total is None else total + term
            acc[:, at] = total if first else acc[:, at] + total

        lax.fori_loop(0, heads * HEAD // wide, tiles, None)

    def turned(t):
        t = t.astype(BF16)
        half = HEAD // 2
        lo, hi = t[:, :half].astype(F32), t[:, half:].astype(F32)
        c, s = cos_s[...], sin_s[...]
        return jnp.concatenate([lo * c - hi * s, hi * c + lo * s], -1).astype(BF16)

    kvw.cross(2)
    qw.mate(0)
    project([z], True)
    kvw.ring(PIECES, far)
    kvw.mate_ring(far)
    qw.ring(early, 2)
    kvw.cross(3)
    kvw.cross(far)
    qw.ring(late, 2)
    qw.ring(early, 3)
    qw.mate_ring(1)
    qw.cross(1)
    qw.mate_ring(2)
    for t in range(far + 1):
        kvw.mate(t)
    kall[me] = turned(_dot(a[...], wkv[:, :HEAD]))
    vall[me] = _dot(a[...], wkv[:, HEAD:]).astype(BF16).T

    bufs = (kall, vall)

    def block(e, ch, ln):
        return bufs[e].at[2 * ch + ln]

    def kv_ring(pieces, t):
        for d, e in pieces:
            @pl.when(t <= hops(d, e))
            def _(d=d, e=e):
                ref = block(e, chip(d, t), lane)
                arrive(ref, zk.at[d, e, t])

                @pl.when(t < hops(d, e))
                def _():
                    remote(ref, sk, zk.at[d, e, t + 1], around[d]).start()

                remote(ref, sd, dk.at[d, e, t], mate).start()

    for d, e in PIECES:
        remote(block(e, z, lane), sk, zk.at[d, e, 1], around[d]).start()
    for e in (0, 1):
        remote(block(e, z, lane), sd, dk.at[0, e, 0], mate).start()
    wo_start()
    qw.mate(1)
    project([chip(0, 1), chip(1, 1)], False)
    qw.ring(late, 3)
    qw.cross(2)
    qw.mate_ring(3)
    qw.ring(early, far)
    qw.mate(2)
    project([chip(0, 2), chip(1, 2)], False)
    qw.cross(3)
    qw.mate_ring(far)
    qw.cross(far)
    qw.mate(3)
    project([chip(0, 3), chip(1, 3)], False)
    qw.mate(far)
    project([chip(0, far)], False)
    kv_ring(early, 1)
    remote(cut(wo, z, lane, 0, rows), so, do.at[0, 0], mate).start()

    def turn_head(h, _):
        at = pl.ds(pl.multiple_of(h * HEAD, HEAD), HEAD)
        qt[h] = turned(acc[:, at]).T

    lax.fori_loop(0, heads, turn_head, None)

    def kv_mate(t):
        for d, e in PIECES:
            cond = (t <= hops(d, e)) if d == 0 else (t > 0) & (t <= hops(d, e))

            @pl.when(cond)
            def _(d=d, e=e):
                arrive(block(e, chip(d, t), 1 - lane), dk.at[d, e, t])

    scale = HEAD**-0.5 * LOG2E
    top[...] = jnp.full(top.shape, NEG, F32)
    mix[...] = jnp.zeros(mix.shape, F32)

    def attend(b, masked):
        keys = kall[b]
        values = jnp.concatenate([vall[b], jnp.ones((8, own), BF16)], axis=0)
        if masked:
            ok = lax.broadcasted_iota(jnp.int32, (own, own), 1) >= lax.broadcasted_iota(jnp.int32, (own, own), 0)
        ahead = 2
        scores = [_dot(keys, qt[h]) for h in range(ahead)]
        waiting = None
        for h in range(heads):
            if h + ahead < heads:
                scores.append(_dot(keys, qt[h + ahead]))
            s = scores[h]
            if masked:
                s = jnp.where(ok, s, HIDDEN)
            old = top[h : h + 1, :]
            new = jnp.maximum(old, s.max(axis=0, keepdims=True))
            top[h : h + 1, :] = new
            now = (h, jnp.exp2((s - new) * scale).astype(BF16), jnp.exp2((old - new) * scale))
            if waiting:
                i, weights, keep = waiting
                mix[i] = mix[i] * keep + _dot(values, weights)
            waiting = now
        i, weights, keep = waiting
        mix[i] = mix[i] * keep + _dot(values, weights)

    attend(me, True)

    def ring_step(t, _):
        @pl.when(t > 0)
        def _():
            kv_ring(late, t)

        def quarter(i, _):
            @pl.when(i == 2)
            def _():
                kv_mate(t)

                @pl.when(t < far)
                def _():
                    wo_ring(t + 1)

                @pl.when(t > 0)
                def _():
                    wo_cross(t)

            @pl.when((i == 3) & (t > 0))
            def _():
                @pl.when(t < far)
                def _():
                    kv_ring(early, t + 1)

                @pl.when(t > 1)
                def _():
                    wo_fourth(t - 1)

            d, other = lax.rem(i, 2), lax.div(i, 2)
            ln = lane + other * (1 - 2 * lane)
            ch = z - t + d * (2 * t - ring)
            near = (d == 0) & (other == 1) & (lane == 1)
            seen_chip = (ch >= 0) & ((d == 0) | (t < far))

            @pl.when(((t == 0) & near) | ((t > 0) & seen_chip))
            def _():
                attend(2 * ch + ln, False)

        lax.fori_loop(0, 4, quarter, None)

    lax.fori_loop(0, far + 1, ring_step, None)

    for h in range(heads):
        total = mix[h, HEAD : HEAD + 1, :]
        seen[:, h * HEAD : (h + 1) * HEAD] = (mix[h, :HEAD, :] * (1 / total)).T.astype(BF16)
    wo_fourth(far)
    arrive(cut(wo, z, 1 - lane, 0, rows), do.at[0, 0])
    for t in range(1, far + 1):
        for d in (0, 1) if t < far else (0,):
            arrive(cut(wo, chip(d, t), 1 - lane, 0, rows), do.at[d, t])
    n_out = depth // wide

    def out_copy(n):
        at = pl.ds(pl.multiple_of(n * wide, wide), wide)
        return pltpu.make_async_copy(a.at[:, at], y_hbm.at[:, at], out_sem.at[n])

    def finish(n, _):
        at = pl.ds(pl.multiple_of(n * wide, wide), wide)
        a[:, at] = (xs[:, at].astype(F32) + _dot(seen[...], wo[:, at])).astype(BF16)
        out_copy(n).start()

    lax.fori_loop(0, n_out, finish, None)
    drain(wkv, skv)
    drain(wq, sq)
    drain(wo, so)
    remote(kall.at[pl.ds(0, 2 * (2 * far - 1))], sk, sk, mate).wait_send()
    remote(kall, sd, sd, mate).wait_send()
    for n in range(n_out):
        out_copy(n).wait()


def solution(mesh):
    side = math.isqrt(mesh.shape["dp"])
    nd = mesh.shape["sp"]
    steps = nd // 4 + 1

    def step(x, gain, wq, wk, wv, wo):
        own, depth = x.shape
        heads = wq.shape[1] // HEAD
        anywhere = pl.BlockSpec(memory_space=pl.ANY)
        vmem = pl.BlockSpec(memory_space=pltpu.VMEM)
        dma = pltpu.SemaphoreType.DMA
        flops = 2 * own * depth * (heads + 2) * HEAD + 2 * own * heads * HEAD * depth + 4 * own * own * nd * heads * HEAD // 2
        halves = [dma((2, 2, steps)), dma((2, 2, steps)), dma((2, 2, steps)), dma]
        return pl.pallas_call(
            functools.partial(_kernel, side),
            out_shape=jax.ShapeDtypeStruct(x.shape, x.dtype),
            in_specs=[anywhere, vmem, anywhere, anywhere, anywhere, anywhere],
            out_specs=anywhere,
            scratch_shapes=[
                pltpu.VMEM((depth, 2 * HEAD), BF16),
                pltpu.VMEM((depth, heads * HEAD), BF16),
                pltpu.VMEM((heads * HEAD, depth), BF16),
                pltpu.VMEM((nd, own, HEAD), BF16),
                pltpu.VMEM((nd, HEAD, own), BF16),
                pltpu.VMEM((own, depth), BF16),
                pltpu.VMEM((own, depth), BF16),
                pltpu.VMEM((own, heads * HEAD), F32),
                pltpu.VMEM((heads, HEAD, own), BF16),
                pltpu.VMEM((heads, HEAD + 8, own), F32),
                pltpu.VMEM((heads, own), F32),
                pltpu.VMEM((own, heads * HEAD), BF16),
                pltpu.VMEM((own, HEAD // 2), F32),
                pltpu.VMEM((own, HEAD // 2), F32),
                dma((5,)),
                *halves,
                *halves,
                dma((2, 2, steps)), dma((2, 2, 2, steps)), dma((2, 2, steps)), dma((2, steps)), dma,
                dma((2, 2, steps)), dma((2, 2, steps)), dma, dma,
                dma((depth // 512,)),
            ],
            compiler_params=pltpu.CompilerParams(collective_id=0, has_side_effects=True, vmem_limit_bytes=VMEM_LIMIT),
            cost_estimate=pl.CostEstimate(flops=flops, bytes_accessed=4 * x.size * 2, transcendentals=own * own * nd * heads // 2),
        )(x, gain, wq, wk, wv, wo)

    tokens, whole = P(("dp", "sp"), None), P("sp", None)
    return jax.shard_map(
        step,
        mesh=mesh,
        in_specs=(tokens, P(None), whole, whole, whole, whole),
        out_specs=tokens,
        check_vma=False,
    )
```

```python
import functools
import math

import jax
import jax.numpy as jnp
from jax import lax
from jax.experimental import pallas as pl
from jax.experimental.pallas import tpu as pltpu
from jax.sharding import PartitionSpec as P

HEAD = 256
THETA = 10000
NEG = -1e30
HIDDEN = 2 * NEG
LOG2E = 1.4426950408889634
MESH = pl.DeviceIdType.MESH
VMEM_LIMIT = 67_043_328
F32, BF16 = jnp.float32, jnp.bfloat16
PIECES = ((0, 0), (1, 1), (0, 1), (1, 0))


def _dot(a, b):
    return lax.dot_general(a, b, (((1,), (0,)), ((), ())), preferred_element_type=F32)


def _kernel(side, x_hbm, gain_ref, wq_hbm, wk_hbm, wv_hbm, wo_hbm, y_hbm, wkv, wq, wo, kall, vall, xs, a, acc, qt, mix, top, seen, cos_s, sin_s,
            local, zkv, xkv, dkv, skv, zq, xq, dq, sq, zo, xo, go, do, so, zk, dk, sk, sd, out_sem):
    own, depth = xs.shape
    nd = kall.shape[0]
    ring = nd // 2
    far = ring // 2
    heads = qt.shape[0]
    rows = depth // nd

    me, dp = lax.axis_index("sp"), lax.axis_index("dp")
    z, lane = lax.div(me, 2), lax.rem(me, 2)
    gx, gy = lax.div(dp, side), lax.rem(dp, side)
    px, py = lax.rem(gx, 2), lax.rem(gy, 2)
    par = lax.rem(px + py, 2)
    around = ((dp, 2 * lax.rem(z + 1, ring) + lane), (dp, 2 * lax.rem(z + ring - 1, ring) + lane))
    partner = ((dp + (1 - 2 * px) * side, me), (dp + 1 - 2 * py, me))
    mate = (dp, 2 * z + 1 - lane)

    def hops(d, e):
        return far if d == e else far - 1

    def chip(d, t):
        return lax.rem(z + ring - t, ring) if d == 0 else lax.rem(z + t, ring)

    def remote(ref, send, recv, to):
        return pltpu.make_async_remote_copy(src_ref=ref, dst_ref=ref, send_sem=send, recv_sem=recv, device_id=to, device_id_type=MESH)

    def arrive(ref, recv):
        remote(ref, recv, recv, mate).wait_recv()

    def cut(w, ch, ln, at, size):
        return w.at[pl.ds(pl.multiple_of((2 * ch + ln) * rows + at, size), size), :]

    class Halves:
        def __init__(self, w, zs, xs_, ds, ss):
            self.w, self.zs, self.xs, self.ds, self.ss = w, zs, xs_, ds, ss

        def part(self, ch, half, e):
            return cut(self.w, ch, lane, half * (rows // 2) + e * (rows // 4), rows // 4)

        def to_mate(self, ch, at, size, t):
            sem = self.ds.at[t] if len(self.ds.shape) else self.ds
            remote(cut(self.w, ch, lane, at, size), self.ss, sem, mate).start()

        def start(self, pieces):
            for d, e in pieces:
                remote(self.part(z, par, e), self.ss, self.zs.at[d, e, 0], around[d]).start()

        def start_mate(self):
            self.to_mate(z, 0, rows, 0)

        def ring(self, pieces, t):
            for d, e in pieces:
                if t <= hops(d, e):
                    ref = self.part(chip(d, t), par, e)
                    arrive(ref, self.zs.at[d, e, t - 1])
                    if t < hops(d, e):
                        remote(ref, self.ss, self.zs.at[d, e, t], around[d]).start()
                    remote(ref, self.ss, self.xs.at[t - 1], partner[e]).start()

        def mate_ring(self, t):
            for d in (0, 1) if t < far else (0,):
                self.to_mate(chip(d, t), par * (rows // 2), rows // 2, t)

        def cross(self, t):
            chips = (0, 1) if t < far else (0,)
            arrive(self.w.at[pl.ds(0, len(chips) * (rows // 2)), :], self.xs.at[t - 1])
            for d in chips:
                self.to_mate(chip(d, t), (1 - par) * (rows // 2), rows // 2, t)

        def mate(self, t):
            arrive(self.w.at[pl.ds(0, (2 if 0 < t < far else 1) * rows), :], self.ds.at[t])

        def mate_all(self):
            arrive(self.w.at[pl.ds(0, nd // 2 * rows), :], self.ds)

    def drain(w, ss):
        total = (2 * far - 1) * rows + nd * rows // 2
        remote(w.at[pl.ds(0, total), :], ss, ss, mate).wait_send()

    kvw, qw = Halves(wkv, zkv, xkv, dkv, skv), Halves(wq, zq, xq, dq, sq)
    early, late = PIECES[:2], PIECES[2:]

    quarter_of = (2 * px + py, 2 * (1 - px) + py, 2 * px + 1 - py, 2 * (1 - px) + 1 - py)

    def out_part(ch, which, e):
        return cut(wo, ch, lane, quarter_of[which] * (rows // 4) + e * (rows // 8), rows // 8)

    def wo_start():
        for d, e in PIECES:
            remote(out_part(z, 0, e), so, zo.at[0], around[d]).start()

    def some(t, whole):
        pl.when(t < far)(lambda: whole(2))
        pl.when(t == far)(lambda: whole(1))

    def wo_ring(t):
        some(t, lambda n: arrive(wo.at[pl.ds(0, n * (rows // 4)), :], zo.at[t - 1]))
        for d, e in PIECES:
            @pl.when(t <= hops(d, e))
            def _(d=d, e=e):
                ref = out_part(chip(d, t), 0, e)

                @pl.when(t < hops(d, e))
                def _():
                    remote(ref, so, zo.at[t], around[d]).start()

                for p in (0, 1):
                    remote(ref, so, xo.at[t - 1], partner[p]).start()

    def wo_cross(t):
        some(t, lambda n: arrive(wo.at[pl.ds(0, n * (rows // 2)), :], xo.at[t - 1]))
        for d, e in PIECES:
            @pl.when(t <= hops(d, e))
            def _(d=d, e=e):
                remote(out_part(chip(d, t), 1 + e, e), so, go.at[t - 1], partner[1 - e]).start()

    def wo_mate(ch):
        remote(cut(wo, ch, lane, 0, rows), so, do, mate).start()

    def wo_fourth(t):
        some(t, lambda n: arrive(wo.at[pl.ds(0, n * (rows // 4)), :], go.at[t - 1]))
        wo_mate(chip(0, t))
        pl.when(t < far)(lambda: wo_mate(chip(1, t)))

    barrier = pltpu.get_barrier_semaphore()
    for to in (*around, *partner, mate):
        pl.semaphore_signal(barrier, inc=1, device_id=to, device_id_type=MESH)
    mine = pl.ds(pl.multiple_of(me * rows, rows), rows)
    loads = [
        pltpu.make_async_copy(wk_hbm, wkv.at[mine, pl.ds(0, HEAD)], local.at[0]),
        pltpu.make_async_copy(wv_hbm, wkv.at[mine, pl.ds(HEAD, HEAD)], local.at[0]),
        pltpu.make_async_copy(wq_hbm, wq.at[mine, :], local.at[1]),
        pltpu.make_async_copy(x_hbm, xs, local.at[2]),
        pltpu.make_async_copy(wo_hbm, wo.at[mine, :], local.at[3]),
    ]
    for load in loads:
        load.start()
    pltpu.make_async_copy(wkv.at[mine, :], wkv.at[mine, :], local.at[0]).wait()
    pl.semaphore_wait(barrier, 5)
    kvw.start(PIECES)
    kvw.start_mate()
    loads[2].wait()
    qw.start(early)
    qw.start_mate()
    loads[3].wait()

    tile = 64
    freq = jnp.exp(lax.broadcasted_iota(jnp.int32, (1, HEAD // 2), 1).astype(F32) * (-math.log(THETA) / (HEAD // 2)))

    def norm(i, _):
        at = pl.ds(pl.multiple_of(i * tile, tile), tile)
        wide = xs[at, :].astype(F32)
        scale = lax.rsqrt(jnp.mean(wide * wide, -1, keepdims=True) + 1e-6)
        a[at, :] = (wide * scale * gain_ref[...].reshape(1, depth).astype(F32)).astype(BF16)

    def angles(i, _):
        at = pl.ds(pl.multiple_of(i * tile, tile), tile)
        place = (lax.broadcasted_iota(jnp.int32, (tile, HEAD // 2), 0) + (me * own + i * tile)).astype(F32)
        angle = place * freq
        cos_s[at, :] = jnp.cos(angle)
        sin_s[at, :] = jnp.sin(angle)

    lax.fori_loop(0, own // tile, norm, None)
    kvw.ring(PIECES, 1)
    qw.start(late)
    kvw.mate_ring(1)
    lax.fori_loop(0, own // tile, angles, None)
    kvw.ring(PIECES, 2)
    kvw.mate_ring(2)
    qw.ring(early, 1)
    loads[4].wait()
    kvw.cross(1)
    kvw.ring(PIECES, 3)
    kvw.mate_ring(3)
    qw.ring(late, 1)

    wide = 512

    def project(chips, first):
        def tiles(n, _):
            at = pl.ds(pl.multiple_of(n * wide, wide), wide)
            total = None
            for ch in chips:
                deep = pl.ds(pl.multiple_of(ch * 2 * rows, 2 * rows), 2 * rows)
                term = _dot(a[:, deep], wq[deep, at])
                total = term if total is None else total + term
            acc[:, at] = total if first else acc[:, at] + total

        lax.fori_loop(0, heads * HEAD // wide, tiles, None)

    def turned(t):
        t = t.astype(BF16)
        half = HEAD // 2
        lo, hi = t[:, :half].astype(F32), t[:, half:].astype(F32)
        c, s = cos_s[...], sin_s[...]
        return jnp.concatenate([lo * c - hi * s, hi * c + lo * s], -1).astype(BF16)

    kvw.cross(2)
    qw.mate(0)
    project([z], True)
    kvw.ring(PIECES, far)
    kvw.mate_ring(far)
    qw.ring(early, 2)
    kvw.cross(3)
    kvw.cross(far)
    qw.ring(late, 2)
    qw.ring(early, 3)
    qw.mate_ring(1)
    qw.cross(1)
    qw.mate_ring(2)
    kvw.mate_all()
    kall[me] = turned(_dot(a[...], wkv[:, :HEAD]))
    vall[me] = _dot(a[...], wkv[:, HEAD:]).astype(BF16).T

    bufs = (kall, vall)

    def block(e, ch, ln):
        return bufs[e].at[2 * ch + ln]

    def kv_ring(pieces, t):
        for d, e in pieces:
            @pl.when(t <= hops(d, e))
            def _(d=d, e=e):
                ref = block(e, chip(d, t), lane)
                arrive(ref, zk.at[d, e, t - 1])

                @pl.when(t < hops(d, e))
                def _():
                    remote(ref, sk, zk.at[d, e, t], around[d]).start()

                remote(ref, sd, dk.at[t], mate).start()

    for d, e in PIECES:
        remote(block(e, z, lane), sk, zk.at[d, e, 0], around[d]).start()
    for e in (0, 1):
        remote(block(e, z, lane), sd, dk.at[0], mate).start()
    wo_start()
    qw.ring(late, 3)
    qw.mate_ring(3)
    qw.cross(2)
    qw.mate(1)
    qw.ring(early, far)
    qw.mate_ring(far)
    project([chip(0, 1), chip(1, 1)], False)
    qw.cross(3)
    qw.mate(2)
    project([chip(0, 2), chip(1, 2)], False)
    qw.mate(3)
    project([chip(0, 3), chip(1, 3)], False)
    qw.cross(far)
    qw.mate(far)
    project([chip(0, far)], False)
    kv_ring(early, 1)
    wo_mate(z)

    def turn_head(h, _):
        at = pl.ds(pl.multiple_of(h * HEAD, HEAD), HEAD)
        qt[h] = turned(acc[:, at]).T

    lax.fori_loop(0, heads, turn_head, None)

    def kv_mate(t):
        both = (t > 0) & (t < far)
        pl.when(both)(lambda: arrive(kall.at[pl.ds(0, 4)], dk.at[t]))
        pl.when(jnp.logical_not(both))(lambda: arrive(kall.at[pl.ds(0, 2)], dk.at[t]))

    scale = HEAD**-0.5 * LOG2E
    group = 4

    def attend_own():
        half = own // 2
        values = jnp.concatenate([vall[me], jnp.ones((8, own), BF16)], axis=0)
        ok = lax.broadcasted_iota(jnp.int32, (half, half), 1) >= lax.broadcasted_iota(jnp.int32, (half, half), 0)
        for g in range(0, heads, group):
            scores = [(_dot(kall[me, :half, :], qt[h, :, :half]), _dot(kall[me], qt[h, :, half:])) for h in range(g, g + group)]
            weights = []
            for h, (low, high) in enumerate(scores, g):
                low = jnp.where(ok, low, HIDDEN)
                high = jnp.concatenate([high[:half], jnp.where(ok, high[half:], HIDDEN)], axis=0)
                tops = [part.max(axis=0, keepdims=True) for part in (low, high)]
                top[h : h + 1, :] = jnp.concatenate(tops, axis=1)
                weights.append([jnp.exp2((part - new) * scale).astype(BF16) for part, new in zip((low, high), tops)])
            for h, (low, high) in enumerate(weights, g):
                mix[h, :, :half] = _dot(values[:, :half], low)
                mix[h, :, half:] = _dot(values, high)

    def settle(h, total):
        seen[:, h * HEAD : (h + 1) * HEAD] = (total[:HEAD] * (1 / total[HEAD : HEAD + 1])).T.astype(BF16)

    def attend(blocks, last=False):
        values = [jnp.concatenate([vall[b], jnp.ones((8, own), BF16)], axis=0) for b in blocks]
        scores, ready = {}, {}

        def score(h):
            scores[h] = [_dot(kall[b], qt[h]) for b in blocks]

        def soften(h):
            ss = scores.pop(h)
            old = top[h : h + 1, :]
            new = functools.reduce(jnp.maximum, [s.max(axis=0, keepdims=True) for s in ss], old)
            top[h : h + 1, :] = new
            ready[h] = [jnp.exp2((s - new) * scale).astype(BF16) for s in ss], jnp.exp2((old - new) * scale)

        def gather(h):
            weights, keep = ready.pop(h)
            total = mix[h] * keep + sum(_dot(v, w) for v, w in zip(values, weights))
            if last:
                settle(h, total)
            else:
                mix[h] = total

        for g in range(0, heads, group):
            for stage in (score, soften, gather):
                for h in range(g, g + group):
                    stage(h)

    attend_own()

    def ring_step(t, _):
        @pl.when(t > 0)
        def _():
            kv_ring(late, t)

        def half_step(other, _):
            @pl.when((other == 0) & (t == far))
            def _():
                wo_cross(far)
                wo_fourth(far - 1)

            @pl.when(other == 1)
            def _():
                @pl.when(t < far)
                def _():
                    wo_ring(t + 1)

                @pl.when((t > 0) & (t < far))
                def _():
                    kv_ring(early, t + 1)
                    wo_cross(t)

                @pl.when((t > 1) & (t < far))
                def _():
                    wo_fourth(t - 1)

                pl.when(t == far)(lambda: wo_fourth(far))
                kv_mate(t)

            ln = lane + other * (1 - 2 * lane)
            below, above = z - t, z + t - ring
            middle = (t > 0) & (t < far)
            two = middle & (above >= 0)
            one = (middle & (below >= 0) & (above < 0)) | ((t == 0) & (other == 1) & (lane == 1)) | ((t == far) & (other == 0) & (below >= 0))
            pl.when(two)(lambda: attend([2 * below + ln, 2 * above + ln]))
            pl.when(one)(lambda: attend([2 * below + ln]))

        lax.fori_loop(0, 2, half_step, None)

    lax.fori_loop(0, far + 1, ring_step, None)

    pl.when(z >= far)(lambda: attend([2 * (z - far) + 1 - lane], last=True))

    @pl.when(z < far)
    def _():
        for h in range(heads):
            settle(h, mix[h])

    arrive(wo.at[pl.ds(0, nd // 2 * rows), :], do)
    n_out = depth // wide

    def out_copy(n):
        at = pl.ds(pl.multiple_of(n * wide, wide), wide)
        return pltpu.make_async_copy(a.at[:, at], y_hbm.at[:, at], out_sem.at[n])

    def finish(n, _):
        at = pl.ds(pl.multiple_of(n * wide, wide), wide)
        a[:, at] = (xs[:, at].astype(F32) + _dot(seen[...], wo[:, at])).astype(BF16)
        out_copy(n).start()

    lax.fori_loop(0, n_out, finish, None)
    drain(wkv, skv)
    drain(wq, sq)
    drain(wo, so)
    remote(kall.at[pl.ds(0, 2 * (2 * far - 1))], sk, sk, mate).wait_send()
    remote(kall, sd, sd, mate).wait_send()
    for n in range(n_out):
        out_copy(n).wait()


def solution(mesh):
    side = math.isqrt(mesh.shape["dp"])
    nd = mesh.shape["sp"]
    steps = nd // 4

    def step(x, gain, wq, wk, wv, wo):
        own, depth = x.shape
        heads = wq.shape[1] // HEAD
        anywhere = pl.BlockSpec(memory_space=pl.ANY)
        vmem = pl.BlockSpec(memory_space=pltpu.VMEM)
        dma = pltpu.SemaphoreType.DMA
        flops = 2 * own * depth * (heads + 2) * HEAD + 2 * own * heads * HEAD * depth + 4 * own * own * nd * heads * HEAD // 2
        ring = dma((2, 2, steps))
        return pl.pallas_call(
            functools.partial(_kernel, side),
            out_shape=jax.ShapeDtypeStruct(x.shape, x.dtype),
            in_specs=[anywhere, vmem, anywhere, anywhere, anywhere, anywhere],
            out_specs=anywhere,
            scratch_shapes=[
                pltpu.VMEM((depth, 2 * HEAD), BF16),
                pltpu.VMEM((depth, heads * HEAD), BF16),
                pltpu.VMEM((heads * HEAD, depth), BF16),
                pltpu.VMEM((nd, own, HEAD), BF16),
                pltpu.VMEM((nd, HEAD, own), BF16),
                pltpu.VMEM((own, depth), BF16),
                pltpu.VMEM((own, depth), BF16),
                pltpu.VMEM((own, heads * HEAD), F32),
                pltpu.VMEM((heads, HEAD, own), BF16),
                pltpu.VMEM((heads, HEAD + 8, own), F32),
                pltpu.VMEM((heads, own), F32),
                pltpu.VMEM((own, heads * HEAD), BF16),
                pltpu.VMEM((own, HEAD // 2), F32),
                pltpu.VMEM((own, HEAD // 2), F32),
                dma((4,)),
                ring, dma((steps,)), dma, dma,
                ring, dma((steps,)), dma((steps + 1,)), dma,
                dma((steps,)), dma((steps,)), dma((steps,)), dma, dma,
                ring, dma((steps + 1,)), dma, dma,
                dma((depth // 512,)),
            ],
            compiler_params=pltpu.CompilerParams(collective_id=0, has_side_effects=True, vmem_limit_bytes=VMEM_LIMIT),
            cost_estimate=pl.CostEstimate(flops=flops, bytes_accessed=4 * x.size * 2, transcendentals=own * own * nd * heads // 2),
        )(x, gain, wq, wk, wv, wo)

    tokens, whole = P(("dp", "sp"), None), P("sp", None)
    return jax.shard_map(
        step,
        mesh=mesh,
        in_specs=(tokens, P(None), whole, whole, whole, whole),
        out_specs=tokens,
        check_vma=False,
    )
```

```python
import functools
import math

import jax
import jax.numpy as jnp
from jax import lax
from jax.experimental import pallas as pl
from jax.experimental.pallas import tpu as pltpu
from jax.sharding import PartitionSpec as P

HEAD = 256
THETA = 10000
NEG = -1e30
HIDDEN = 2 * NEG
LOG2E = 1.4426950408889634
MESH = pl.DeviceIdType.MESH
VMEM_LIMIT = 67_043_328
F32, BF16 = jnp.float32, jnp.bfloat16
PIECES = ((0, 0), (1, 1), (0, 1), (1, 0))


def _dot(a, b):
    return lax.dot_general(a, b, (((1,), (0,)), ((), ())), preferred_element_type=F32)


def _kernel(side, x_hbm, gain_ref, wq_hbm, wk_hbm, wv_hbm, wo_hbm, y_hbm, wkv, wq, wo, kall, vall, xs, a, acc, qt, mix, top, seen, cos_s, sin_s,
            local, zkv, xkv, dkv, skv, zq, xq, dq, sq, zo, xo, go, do, so, zk, dk, sk, sd, out_sem):
    own, depth = xs.shape
    nd = kall.shape[0]
    ring = nd // 2
    far = ring // 2
    heads = qt.shape[0]
    rows = depth // nd

    me, dp = lax.axis_index("sp"), lax.axis_index("dp")
    z, lane = lax.div(me, 2), lax.rem(me, 2)
    gx, gy = lax.div(dp, side), lax.rem(dp, side)
    px, py = lax.rem(gx, 2), lax.rem(gy, 2)
    par = lax.rem(px + py, 2)
    around = ((dp, 2 * lax.rem(z + 1, ring) + lane), (dp, 2 * lax.rem(z + ring - 1, ring) + lane))
    partner = ((dp + (1 - 2 * px) * side, me), (dp + 1 - 2 * py, me))
    mate = (dp, 2 * z + 1 - lane)

    def hops(d, e):
        return far if d == e else far - 1

    def chip(d, t):
        return lax.rem(z + ring - t, ring) if d == 0 else lax.rem(z + t, ring)

    def remote(ref, send, recv, to):
        return pltpu.make_async_remote_copy(src_ref=ref, dst_ref=ref, send_sem=send, recv_sem=recv, device_id=to, device_id_type=MESH)

    def arrive(ref, recv):
        remote(ref, recv, recv, mate).wait_recv()

    def cut(w, ch, ln, at, size):
        return w.at[pl.ds(pl.multiple_of((2 * ch + ln) * rows + at, size), size), :]

    class Halves:
        def __init__(self, w, zs, xs_, ds, ss):
            self.w, self.zs, self.xs, self.ds, self.ss = w, zs, xs_, ds, ss

        def part(self, ch, half, e):
            return cut(self.w, ch, lane, half * (rows // 2) + e * (rows // 4), rows // 4)

        def to_mate(self, ch, at, size, t):
            sem = self.ds.at[t] if len(self.ds.shape) else self.ds
            remote(cut(self.w, ch, lane, at, size), self.ss, sem, mate).start()

        def start(self, pieces):
            for d, e in pieces:
                remote(self.part(z, par, e), self.ss, self.zs.at[d, e, 0], around[d]).start()

        def start_mate(self):
            self.to_mate(z, 0, rows, 0)

        def ring(self, pieces, t):
            for d, e in pieces:
                if t <= hops(d, e):
                    ref = self.part(chip(d, t), par, e)
                    arrive(ref, self.zs.at[d, e, t - 1])
                    if t < hops(d, e):
                        remote(ref, self.ss, self.zs.at[d, e, t], around[d]).start()
                    remote(ref, self.ss, self.xs.at[t - 1], partner[e]).start()

        def mate_ring(self, t):
            for d in (0, 1) if t < far else (0,):
                self.to_mate(chip(d, t), par * (rows // 2), rows // 2, t)

        def cross(self, t):
            chips = (0, 1) if t < far else (0,)
            arrive(self.w.at[pl.ds(0, len(chips) * (rows // 2)), :], self.xs.at[t - 1])
            for d in chips:
                self.to_mate(chip(d, t), (1 - par) * (rows // 2), rows // 2, t)

        def mate(self, t):
            arrive(self.w.at[pl.ds(0, (2 if 0 < t < far else 1) * rows), :], self.ds.at[t])

        def mate_all(self):
            arrive(self.w.at[pl.ds(0, nd // 2 * rows), :], self.ds)

    def drain(w, ss):
        total = (2 * far - 1) * rows + nd * rows // 2
        remote(w.at[pl.ds(0, total), :], ss, ss, mate).wait_send()

    kvw, qw = Halves(wkv, zkv, xkv, dkv, skv), Halves(wq, zq, xq, dq, sq)
    early, late = PIECES[:2], PIECES[2:]

    quarter_of = (2 * px + py, 2 * (1 - px) + py, 2 * px + 1 - py, 2 * (1 - px) + 1 - py)

    def out_part(ch, which, e):
        return cut(wo, ch, lane, quarter_of[which] * (rows // 4) + e * (rows // 8), rows // 8)

    def wo_start():
        for d, e in PIECES:
            remote(out_part(z, 0, e), so, zo.at[0], around[d]).start()

    def some(t, whole):
        pl.when(t < far)(lambda: whole(2))
        pl.when(t == far)(lambda: whole(1))

    def wo_ring(t):
        some(t, lambda n: arrive(wo.at[pl.ds(0, n * (rows // 4)), :], zo.at[t - 1]))
        for d, e in PIECES:
            @pl.when(t <= hops(d, e))
            def _(d=d, e=e):
                ref = out_part(chip(d, t), 0, e)

                @pl.when(t < hops(d, e))
                def _():
                    remote(ref, so, zo.at[t], around[d]).start()

                for p in (0, 1):
                    remote(ref, so, xo.at[t - 1], partner[p]).start()

    def wo_cross(t):
        some(t, lambda n: arrive(wo.at[pl.ds(0, n * (rows // 2)), :], xo.at[t - 1]))
        for d, e in PIECES:
            @pl.when(t <= hops(d, e))
            def _(d=d, e=e):
                remote(out_part(chip(d, t), 1 + e, e), so, go.at[t - 1], partner[1 - e]).start()

    def wo_mate(ch):
        remote(cut(wo, ch, lane, 0, rows), so, do, mate).start()

    def wo_fourth(t):
        some(t, lambda n: arrive(wo.at[pl.ds(0, n * (rows // 4)), :], go.at[t - 1]))
        wo_mate(chip(0, t))
        pl.when(t < far)(lambda: wo_mate(chip(1, t)))

    barrier = pltpu.get_barrier_semaphore()
    for to in (*around, *partner, mate):
        pl.semaphore_signal(barrier, inc=1, device_id=to, device_id_type=MESH)
    mine = pl.ds(pl.multiple_of(me * rows, rows), rows)
    loads = [
        pltpu.make_async_copy(wk_hbm, wkv.at[mine, pl.ds(0, HEAD)], local.at[0]),
        pltpu.make_async_copy(wv_hbm, wkv.at[mine, pl.ds(HEAD, HEAD)], local.at[0]),
        pltpu.make_async_copy(wq_hbm, wq.at[mine, :], local.at[1]),
        pltpu.make_async_copy(x_hbm, xs, local.at[2]),
        pltpu.make_async_copy(wo_hbm, wo.at[mine, :], local.at[3]),
    ]
    for load in loads:
        load.start()
    pltpu.make_async_copy(wkv.at[mine, :], wkv.at[mine, :], local.at[0]).wait()
    pl.semaphore_wait(barrier, 5)
    kvw.start(PIECES)
    kvw.start_mate()
    loads[2].wait()
    qw.start(early)
    qw.start_mate()
    loads[3].wait()

    tile = 64
    freq = jnp.exp(lax.broadcasted_iota(jnp.int32, (1, HEAD // 2), 1).astype(F32) * (-math.log(THETA) / (HEAD // 2)))

    def norm(i, _):
        at = pl.ds(pl.multiple_of(i * tile, tile), tile)
        wide = xs[at, :].astype(F32)
        scale = lax.rsqrt(jnp.mean(wide * wide, -1, keepdims=True) + 1e-6)
        a[at, :] = (wide * scale * gain_ref[...].reshape(1, depth).astype(F32)).astype(BF16)

    def angles(i, _):
        at = pl.ds(pl.multiple_of(i * tile, tile), tile)
        place = (lax.broadcasted_iota(jnp.int32, (tile, HEAD // 2), 0) + (me * own + i * tile)).astype(F32)
        angle = place * freq
        cos_s[at, :] = jnp.cos(angle)
        sin_s[at, :] = jnp.sin(angle)

    lax.fori_loop(0, own // tile, norm, None)
    kvw.ring(PIECES, 1)
    qw.start(late)
    kvw.mate_ring(1)
    lax.fori_loop(0, own // tile, angles, None)
    kvw.ring(PIECES, 2)
    kvw.mate_ring(2)
    qw.ring(early, 1)
    loads[4].wait()
    kvw.cross(1)
    kvw.ring(PIECES, 3)
    kvw.mate_ring(3)
    qw.ring(late, 1)

    wide = 512

    def project(chips, first):
        def tiles(n, _):
            at = pl.ds(pl.multiple_of(n * wide, wide), wide)
            total = None
            for ch in chips:
                deep = pl.ds(pl.multiple_of(ch * 2 * rows, 2 * rows), 2 * rows)
                term = _dot(a[:, deep], wq[deep, at])
                total = term if total is None else total + term
            acc[:, at] = total if first else acc[:, at] + total

        lax.fori_loop(0, heads * HEAD // wide, tiles, None)

    def turned(t):
        t = t.astype(BF16)
        half = HEAD // 2
        lo, hi = t[:, :half].astype(F32), t[:, half:].astype(F32)
        c, s = cos_s[...], sin_s[...]
        return jnp.concatenate([lo * c - hi * s, hi * c + lo * s], -1).astype(BF16)

    kvw.cross(2)
    qw.mate(0)
    project([z], True)
    kvw.ring(PIECES, far)
    kvw.mate_ring(far)
    qw.ring(early, 2)
    kvw.cross(3)
    kvw.cross(far)
    qw.ring(late, 2)
    qw.ring(early, 3)
    qw.mate_ring(1)
    qw.cross(1)
    qw.mate_ring(2)
    kvw.mate_all()
    kall[me] = turned(_dot(a[...], wkv[:, :HEAD]))
    vall[me] = _dot(a[...], wkv[:, HEAD:]).astype(BF16).T

    bufs = (kall, vall)

    def block(e, ch, ln):
        return bufs[e].at[2 * ch + ln]

    def kv_ring(pieces, t):
        for d, e in pieces:
            @pl.when(t <= hops(d, e))
            def _(d=d, e=e):
                ref = block(e, chip(d, t), lane)
                arrive(ref, zk.at[d, e, t - 1])

                @pl.when(t < hops(d, e))
                def _():
                    remote(ref, sk, zk.at[d, e, t], around[d]).start()

                remote(ref, sd, dk.at[t], mate).start()

    for d, e in PIECES:
        remote(block(e, z, lane), sk, zk.at[d, e, 0], around[d]).start()
    for e in (0, 1):
        remote(block(e, z, lane), sd, dk.at[0], mate).start()
    wo_start()
    qw.ring(late, 3)
    qw.mate_ring(3)
    qw.cross(2)
    qw.mate(1)
    qw.ring(early, far)
    qw.mate_ring(far)
    project([chip(0, 1), chip(1, 1)], False)
    qw.cross(3)
    qw.mate(2)
    project([chip(0, 2), chip(1, 2)], False)
    qw.cross(far)
    qw.mate(3)
    project([chip(0, 3), chip(1, 3)], False)
    qw.mate(far)
    project([chip(0, far)], False)
    kv_ring(early, 1)
    wo_mate(z)

    def turn_head(h, _):
        at = pl.ds(pl.multiple_of(h * HEAD, HEAD), HEAD)
        qt[h] = turned(acc[:, at]).T

    lax.fori_loop(0, heads, turn_head, None)

    def kv_mate(t):
        both = (t > 0) & (t < far)
        pl.when(both)(lambda: arrive(kall.at[pl.ds(0, 4)], dk.at[t]))
        pl.when(jnp.logical_not(both))(lambda: arrive(kall.at[pl.ds(0, 2)], dk.at[t]))

    scale = HEAD**-0.5 * LOG2E
    group = 4

    def attend_own():
        half = own // 2
        values = jnp.concatenate([vall[me], jnp.ones((8, own), BF16)], axis=0)
        ok = lax.broadcasted_iota(jnp.int32, (half, half), 1) >= lax.broadcasted_iota(jnp.int32, (half, half), 0)
        for g in range(0, heads, group):
            scores = [(_dot(kall[me, :half, :], qt[h, :, :half]), _dot(kall[me], qt[h, :, half:])) for h in range(g, g + group)]
            weights = []
            for h, (low, high) in enumerate(scores, g):
                low = jnp.where(ok, low, HIDDEN)
                high = jnp.concatenate([high[:half], jnp.where(ok, high[half:], HIDDEN)], axis=0)
                tops = [part.max(axis=0, keepdims=True) for part in (low, high)]
                top[h : h + 1, :] = jnp.concatenate(tops, axis=1)
                weights.append([jnp.exp2((part - new) * scale).astype(BF16) for part, new in zip((low, high), tops)])
            for h, (low, high) in enumerate(weights, g):
                mix[h, :, :half] = _dot(values[:, :half], low)
                mix[h, :, half:] = _dot(values, high)

    def settle(h, total):
        seen[:, h * HEAD : (h + 1) * HEAD] = (total[:HEAD] * (1 / total[HEAD : HEAD + 1])).T.astype(BF16)

    def attend(blocks, last=False):
        values = [jnp.concatenate([vall[b], jnp.ones((8, own), BF16)], axis=0) for b in blocks]
        scores, ready = {}, {}

        def score(h):
            scores[h] = [_dot(kall[b], qt[h]) for b in blocks]

        def soften(h):
            ss = scores.pop(h)
            old = top[h : h + 1, :]
            new = functools.reduce(jnp.maximum, [s.max(axis=0, keepdims=True) for s in ss], old)
            top[h : h + 1, :] = new
            ready[h] = [jnp.exp2((s - new) * scale).astype(BF16) for s in ss], jnp.exp2((old - new) * scale)

        def gather(h):
            weights, keep = ready.pop(h)
            total = mix[h] * keep + sum(_dot(v, w) for v, w in zip(values, weights))
            if last:
                settle(h, total)
            else:
                mix[h] = total

        for g in range(0, heads, group):
            for stage in (score, soften, gather):
                for h in range(g, g + group):
                    stage(h)

    attend_own()

    def ring_step(t, _):
        @pl.when(t > 0)
        def _():
            kv_ring(late, t)

        def half_step(other, _):
            @pl.when((other == 0) & (t == far))
            def _():
                wo_cross(far)
                wo_fourth(far - 1)

            @pl.when(other == 1)
            def _():
                @pl.when(t < far)
                def _():
                    wo_ring(t + 1)

                @pl.when((t > 0) & (t < far))
                def _():
                    kv_ring(early, t + 1)
                    wo_cross(t)

                @pl.when((t > 1) & (t < far))
                def _():
                    wo_fourth(t - 1)

                pl.when(t == far)(lambda: wo_fourth(far))
                kv_mate(t)

            ln = lane + other * (1 - 2 * lane)
            below, above = z - t, z + t - ring
            middle = (t > 0) & (t < far)
            two = middle & (above >= 0)
            one = (middle & (below >= 0) & (above < 0)) | ((t == 0) & (other == 1) & (lane == 1)) | ((t == far) & (other == 0) & (below >= 0))
            pl.when(two)(lambda: attend([2 * below + ln, 2 * above + ln]))
            pl.when(one)(lambda: attend([2 * below + ln]))

        lax.fori_loop(0, 2, half_step, None)

    lax.fori_loop(0, far + 1, ring_step, None)

    pl.when(z >= far)(lambda: attend([2 * (z - far) + 1 - lane], last=True))

    @pl.when(z < far)
    def _():
        for h in range(heads):
            settle(h, mix[h])

    arrive(wo.at[pl.ds(0, nd // 2 * rows), :], do)
    n_out = depth // wide

    def out_copy(n):
        at = pl.ds(pl.multiple_of(n * wide, wide), wide)
        return pltpu.make_async_copy(a.at[:, at], y_hbm.at[:, at], out_sem.at[n])

    def finish(n, _):
        at = pl.ds(pl.multiple_of(n * wide, wide), wide)
        a[:, at] = (xs[:, at].astype(F32) + _dot(seen[...], wo[:, at])).astype(BF16)
        out_copy(n).start()

    lax.fori_loop(0, n_out, finish, None)
    drain(wkv, skv)
    drain(wq, sq)
    drain(wo, so)
    remote(kall.at[pl.ds(0, 2 * (2 * far - 1))], sk, sk, mate).wait_send()
    remote(kall, sd, sd, mate).wait_send()
    for n in range(n_out):
        out_copy(n).wait()


def _hand_on(src, dst, buf, into, out):
    strips = into.shape[0]
    size = src.shape[0] // strips
    reads, writes = [], []
    for i in range(strips):
        at = pl.ds(i * size, size)
        reads.append(pltpu.make_async_copy(src.at[at, :], buf.at[at, :], into.at[i]))
        writes.append(pltpu.make_async_copy(buf.at[at, :], dst.at[at, :], out.at[i]))
    for read in reads:
        read.start()
    for read, write in zip(reads, writes):
        read.wait()
        write.start()
    for write in writes:
        write.wait()


def solution(mesh):
    side = math.isqrt(mesh.shape["dp"])
    nd = mesh.shape["sp"]
    steps = nd // 4

    def step(x, gain, wq, wk, wv, wo):
        own, depth = x.shape
        heads = wq.shape[1] // HEAD
        anywhere = pl.BlockSpec(memory_space=pl.ANY)
        vmem = pl.BlockSpec(memory_space=pltpu.VMEM)
        dma = pltpu.SemaphoreType.DMA
        flops = 2 * own * depth * (heads + 2) * HEAD + 2 * own * heads * HEAD * depth + 4 * own * own * nd * heads * HEAD // 2
        ring = dma((2, 2, steps))
        y = pl.pallas_call(
            functools.partial(_kernel, side),
            out_shape=jax.ShapeDtypeStruct(x.shape, x.dtype),
            in_specs=[anywhere, vmem, anywhere, anywhere, anywhere, anywhere],
            out_specs=anywhere,
            scratch_shapes=[
                pltpu.VMEM((depth, 2 * HEAD), BF16),
                pltpu.VMEM((depth, heads * HEAD), BF16),
                pltpu.VMEM((heads * HEAD, depth), BF16),
                pltpu.VMEM((nd, own, HEAD), BF16),
                pltpu.VMEM((nd, HEAD, own), BF16),
                pltpu.VMEM((own, depth), BF16),
                pltpu.VMEM((own, depth), BF16),
                pltpu.VMEM((own, heads * HEAD), F32),
                pltpu.VMEM((heads, HEAD, own), BF16),
                pltpu.VMEM((heads, HEAD + 8, own), F32),
                pltpu.VMEM((heads, own), F32),
                pltpu.VMEM((own, heads * HEAD), BF16),
                pltpu.VMEM((own, HEAD // 2), F32),
                pltpu.VMEM((own, HEAD // 2), F32),
                dma((4,)),
                ring, dma((steps,)), dma, dma,
                ring, dma((steps,)), dma((steps + 1,)), dma,
                dma((steps,)), dma((steps,)), dma((steps,)), dma, dma,
                ring, dma((steps + 1,)), dma, dma,
                dma((depth // 512,)),
            ],
            compiler_params=pltpu.CompilerParams(collective_id=0, has_side_effects=True, vmem_limit_bytes=VMEM_LIMIT),
            cost_estimate=pl.CostEstimate(flops=flops, bytes_accessed=4 * x.size * 2, transcendentals=own * own * nd * heads // 2),
        )(x, gain, wq, wk, wv, wo)
        return pl.pallas_call(
            _hand_on,
            out_shape=jax.ShapeDtypeStruct(x.shape, x.dtype),
            in_specs=[anywhere],
            out_specs=anywhere,
            scratch_shapes=[pltpu.VMEM(x.shape, x.dtype), dma((8,)), dma((8,))],
            compiler_params=pltpu.CompilerParams(vmem_limit_bytes=VMEM_LIMIT),
            cost_estimate=pl.CostEstimate(flops=0, bytes_accessed=4 * x.size, transcendentals=0),
        )(y)

    tokens, whole = P(("dp", "sp"), None), P("sp", None)
    return jax.shard_map(
        step,
        mesh=mesh,
        in_specs=(tokens, P(None), whole, whole, whole, whole),
        out_specs=tokens,
        check_vma=False,
    )
```

```python
import functools
import math

import jax
import jax.numpy as jnp
from jax import lax
from jax.experimental import pallas as pl
from jax.experimental.pallas import tpu as pltpu
from jax.sharding import PartitionSpec as P

HEAD = 256
THETA = 10000
NEG = -1e30
HIDDEN = 2 * NEG
LOG2E = 1.4426950408889634
MESH = pl.DeviceIdType.MESH
VMEM_LIMIT = 67_043_328
F32, BF16 = jnp.float32, jnp.bfloat16
PIECES = ((0, 0), (1, 1), (0, 1), (1, 0))


def _dot(a, b):
    return lax.dot_general(a, b, (((1,), (0,)), ((), ())), preferred_element_type=F32)


def _kernel(side, x_hbm, gain_ref, wq_hbm, wk_hbm, wv_hbm, wo_hbm, y_hbm, wkv, wq, wo, kall, vall, xs, a, acc, qt, mix, top, seen, cos_s, sin_s,
            local, zkv, xkv, dkv, skv, zq, xq, dq, sq, zo, xo, go, do, so, zk, dk, sk, sd, out_sem):
    own, depth = xs.shape
    nd = kall.shape[0]
    ring = nd // 2
    far = ring // 2
    heads = qt.shape[0]
    rows = depth // nd

    me, dp = lax.axis_index("sp"), lax.axis_index("dp")
    z, lane = lax.div(me, 2), lax.rem(me, 2)
    gx, gy = lax.div(dp, side), lax.rem(dp, side)
    px, py = lax.rem(gx, 2), lax.rem(gy, 2)
    par = lax.rem(px + py, 2)
    around = ((dp, 2 * lax.rem(z + 1, ring) + lane), (dp, 2 * lax.rem(z + ring - 1, ring) + lane))
    partner = ((dp + (1 - 2 * px) * side, me), (dp + 1 - 2 * py, me))
    mate = (dp, 2 * z + 1 - lane)

    def hops(d, e):
        return far if d == e else far - 1

    def chip(d, t):
        return lax.rem(z + ring - t, ring) if d == 0 else lax.rem(z + t, ring)

    def remote(ref, send, recv, to):
        return pltpu.make_async_remote_copy(src_ref=ref, dst_ref=ref, send_sem=send, recv_sem=recv, device_id=to, device_id_type=MESH)

    def arrive(ref, recv):
        remote(ref, recv, recv, mate).wait_recv()

    def cut(w, ch, ln, at, size):
        return w.at[pl.ds(pl.multiple_of((2 * ch + ln) * rows + at, size), size), :]

    class Halves:
        def __init__(self, w, zs, xs_, ds, ss):
            self.w, self.zs, self.xs, self.ds, self.ss = w, zs, xs_, ds, ss

        def part(self, ch, half, e):
            return cut(self.w, ch, lane, half * (rows // 2) + e * (rows // 4), rows // 4)

        def to_mate(self, ch, at, size, t):
            sem = self.ds.at[t] if len(self.ds.shape) else self.ds
            remote(cut(self.w, ch, lane, at, size), self.ss, sem, mate).start()

        def start(self, pieces):
            for d, e in pieces:
                remote(self.part(z, par, e), self.ss, self.zs.at[d, e, 0], around[d]).start()

        def start_mate(self):
            self.to_mate(z, 0, rows, 0)

        def ring(self, pieces, t):
            for d, e in pieces:
                if t <= hops(d, e):
                    ref = self.part(chip(d, t), par, e)
                    arrive(ref, self.zs.at[d, e, t - 1])
                    if t < hops(d, e):
                        remote(ref, self.ss, self.zs.at[d, e, t], around[d]).start()
                    remote(ref, self.ss, self.xs.at[t - 1], partner[e]).start()

        def mate_ring(self, t):
            for d in (0, 1) if t < far else (0,):
                self.to_mate(chip(d, t), par * (rows // 2), rows // 2, t)

        def cross(self, t):
            chips = (0, 1) if t < far else (0,)
            arrive(self.w.at[pl.ds(0, len(chips) * (rows // 2)), :], self.xs.at[t - 1])
            for d in chips:
                self.to_mate(chip(d, t), (1 - par) * (rows // 2), rows // 2, t)

        def mate(self, t):
            arrive(self.w.at[pl.ds(0, (2 if 0 < t < far else 1) * rows), :], self.ds.at[t])

        def mate_all(self):
            arrive(self.w.at[pl.ds(0, nd // 2 * rows), :], self.ds)

    def drain(w, ss):
        total = (2 * far - 1) * rows + nd * rows // 2
        remote(w.at[pl.ds(0, total), :], ss, ss, mate).wait_send()

    kvw, qw = Halves(wkv, zkv, xkv, dkv, skv), Halves(wq, zq, xq, dq, sq)
    early, late = PIECES[:2], PIECES[2:]

    quarter_of = (2 * px + py, 2 * (1 - px) + py, 2 * px + 1 - py, 2 * (1 - px) + 1 - py)

    def out_part(ch, which, e):
        return cut(wo, ch, lane, quarter_of[which] * (rows // 4) + e * (rows // 8), rows // 8)

    def wo_start():
        for d, e in PIECES:
            remote(out_part(z, 0, e), so, zo.at[0], around[d]).start()

    def some(t, whole):
        pl.when(t < far)(lambda: whole(2))
        pl.when(t == far)(lambda: whole(1))

    def wo_ring(t):
        some(t, lambda n: arrive(wo.at[pl.ds(0, n * (rows // 4)), :], zo.at[t - 1]))
        for d, e in PIECES:
            @pl.when(t <= hops(d, e))
            def _(d=d, e=e):
                ref = out_part(chip(d, t), 0, e)

                @pl.when(t < hops(d, e))
                def _():
                    remote(ref, so, zo.at[t], around[d]).start()

                for p in (0, 1):
                    remote(ref, so, xo.at[t - 1], partner[p]).start()

    def wo_cross(t):
        some(t, lambda n: arrive(wo.at[pl.ds(0, n * (rows // 2)), :], xo.at[t - 1]))
        for d, e in PIECES:
            @pl.when(t <= hops(d, e))
            def _(d=d, e=e):
                remote(out_part(chip(d, t), 1 + e, e), so, go.at[t - 1], partner[1 - e]).start()

    def wo_mate(ch):
        remote(cut(wo, ch, lane, 0, rows), so, do, mate).start()

    def wo_fourth(t):
        some(t, lambda n: arrive(wo.at[pl.ds(0, n * (rows // 4)), :], go.at[t - 1]))
        wo_mate(chip(0, t))
        pl.when(t < far)(lambda: wo_mate(chip(1, t)))

    barrier = pltpu.get_barrier_semaphore()
    for to in (*around, *partner, mate):
        pl.semaphore_signal(barrier, inc=1, device_id=to, device_id_type=MESH)
    mine = pl.ds(pl.multiple_of(me * rows, rows), rows)
    loads = [
        pltpu.make_async_copy(wk_hbm, wkv.at[mine, pl.ds(0, HEAD)], local.at[0]),
        pltpu.make_async_copy(wv_hbm, wkv.at[mine, pl.ds(HEAD, HEAD)], local.at[0]),
        pltpu.make_async_copy(wq_hbm, wq.at[mine, :], local.at[1]),
        pltpu.make_async_copy(x_hbm, xs, local.at[2]),
        pltpu.make_async_copy(wo_hbm, wo.at[mine, :], local.at[3]),
    ]
    for load in loads:
        load.start()
    pltpu.make_async_copy(wkv.at[mine, :], wkv.at[mine, :], local.at[0]).wait()
    pl.semaphore_wait(barrier, 5)
    kvw.start(PIECES)
    kvw.start_mate()
    loads[2].wait()
    qw.start(early)
    qw.start_mate()
    loads[3].wait()

    tile = 64
    freq = jnp.exp(lax.broadcasted_iota(jnp.int32, (1, HEAD // 2), 1).astype(F32) * (-math.log(THETA) / (HEAD // 2)))

    def norm(i, _):
        at = pl.ds(pl.multiple_of(i * tile, tile), tile)
        wide = xs[at, :].astype(F32)
        scale = lax.rsqrt(jnp.mean(wide * wide, -1, keepdims=True) + 1e-6)
        a[at, :] = (wide * scale * gain_ref[...].reshape(1, depth).astype(F32)).astype(BF16)

    def angles(i, _):
        at = pl.ds(pl.multiple_of(i * tile, tile), tile)
        place = (lax.broadcasted_iota(jnp.int32, (tile, HEAD // 2), 0) + (me * own + i * tile)).astype(F32)
        angle = place * freq
        cos_s[at, :] = jnp.cos(angle)
        sin_s[at, :] = jnp.sin(angle)

    lax.fori_loop(0, own // tile, norm, None)
    kvw.ring(PIECES, 1)
    qw.start(late)
    kvw.mate_ring(1)
    lax.fori_loop(0, own // tile, angles, None)
    kvw.ring(PIECES, 2)
    kvw.mate_ring(2)
    qw.ring(early, 1)
    loads[4].wait()
    kvw.cross(1)
    kvw.ring(PIECES, 3)
    kvw.mate_ring(3)
    qw.ring(late, 1)

    wide = 512

    def project(chips, first):
        def tiles(n, _):
            at = pl.ds(pl.multiple_of(n * wide, wide), wide)
            total = None
            for ch in chips:
                deep = pl.ds(pl.multiple_of(ch * 2 * rows, 2 * rows), 2 * rows)
                term = _dot(a[:, deep], wq[deep, at])
                total = term if total is None else total + term
            acc[:, at] = total if first else acc[:, at] + total

        lax.fori_loop(0, heads * HEAD // wide, tiles, None)

    def turned(t):
        t = t.astype(BF16)
        half = HEAD // 2
        lo, hi = t[:, :half].astype(F32), t[:, half:].astype(F32)
        c, s = cos_s[...], sin_s[...]
        return jnp.concatenate([lo * c - hi * s, hi * c + lo * s], -1).astype(BF16)

    kvw.cross(2)
    qw.mate(0)
    project([z], True)
    kvw.ring(PIECES, far)
    kvw.mate_ring(far)
    qw.ring(early, 2)
    kvw.cross(3)
    kvw.cross(far)
    qw.ring(late, 2)
    qw.ring(early, 3)
    qw.mate_ring(1)
    qw.cross(1)
    qw.mate_ring(2)
    kvw.mate_all()
    kall[me] = turned(_dot(a[...], wkv[:, :HEAD]))
    vall[me] = _dot(a[...], wkv[:, HEAD:]).astype(BF16).T

    bufs = (kall, vall)

    def block(e, ch, ln):
        return bufs[e].at[2 * ch + ln]

    def kv_ring(pieces, t):
        for d, e in pieces:
            @pl.when(t <= hops(d, e))
            def _(d=d, e=e):
                ref = block(e, chip(d, t), lane)
                arrive(ref, zk.at[d, e, t - 1])

                @pl.when(t < hops(d, e))
                def _():
                    remote(ref, sk, zk.at[d, e, t], around[d]).start()

                remote(ref, sd, dk.at[t], mate).start()

    for d, e in PIECES:
        remote(block(e, z, lane), sk, zk.at[d, e, 0], around[d]).start()
    for e in (0, 1):
        remote(block(e, z, lane), sd, dk.at[0], mate).start()
    wo_start()
    qw.ring(late, 3)
    qw.mate_ring(3)
    qw.cross(2)
    qw.mate(1)
    qw.ring(early, far)
    qw.mate_ring(far)
    project([chip(0, 1), chip(1, 1)], False)
    qw.cross(3)
    qw.mate(2)
    project([chip(0, 2), chip(1, 2)], False)
    qw.cross(far)
    qw.mate(3)
    project([chip(0, 3), chip(1, 3)], False)
    qw.mate(far)
    project([chip(0, far)], False)
    kv_ring(early, 1)
    wo_mate(z)

    def turn_head(h, _):
        at = pl.ds(pl.multiple_of(h * HEAD, HEAD), HEAD)
        qt[h] = turned(acc[:, at]).T

    lax.fori_loop(0, heads, turn_head, None)

    def kv_mate(t):
        both = (t > 0) & (t < far)
        pl.when(both)(lambda: arrive(kall.at[pl.ds(0, 4)], dk.at[t]))
        pl.when(jnp.logical_not(both))(lambda: arrive(kall.at[pl.ds(0, 2)], dk.at[t]))

    scale = HEAD**-0.5 * LOG2E
    group = 4

    def attend_own():
        half = own // 2
        values = jnp.concatenate([vall[me], jnp.ones((8, own), BF16)], axis=0)
        ok = lax.broadcasted_iota(jnp.int32, (half, half), 1) >= lax.broadcasted_iota(jnp.int32, (half, half), 0)
        for g in range(0, heads, group):
            scores = [(_dot(kall[me, :half, :], qt[h, :, :half]), _dot(kall[me], qt[h, :, half:])) for h in range(g, g + group)]
            weights = []
            for h, (low, high) in enumerate(scores, g):
                low = jnp.where(ok, low, HIDDEN)
                high = jnp.concatenate([high[:half], jnp.where(ok, high[half:], HIDDEN)], axis=0)
                tops = [part.max(axis=0, keepdims=True) for part in (low, high)]
                top[h : h + 1, :] = jnp.concatenate(tops, axis=1)
                weights.append([jnp.exp2((part - new) * scale).astype(BF16) for part, new in zip((low, high), tops)])
            for h, (low, high) in enumerate(weights, g):
                mix[h, :, :half] = _dot(values[:, :half], low)
                mix[h, :, half:] = _dot(values, high)

    def settle(h, total):
        seen[:, h * HEAD : (h + 1) * HEAD] = (total[:HEAD] * (1 / total[HEAD : HEAD + 1])).T.astype(BF16)

    def attend(blocks, last=False):
        values = [jnp.concatenate([vall[b], jnp.ones((8, own), BF16)], axis=0) for b in blocks]
        scores, ready = {}, {}

        def score(h):
            scores[h] = [_dot(kall[b], qt[h]) for b in blocks]

        def soften(h):
            ss = scores.pop(h)
            old = top[h : h + 1, :]
            new = functools.reduce(jnp.maximum, [s.max(axis=0, keepdims=True) for s in ss], old)
            top[h : h + 1, :] = new
            ready[h] = [jnp.exp2((s - new) * scale).astype(BF16) for s in ss], jnp.exp2((old - new) * scale)

        def gather(h):
            weights, keep = ready.pop(h)
            total = mix[h] * keep + sum(_dot(v, w) for v, w in zip(values, weights))
            if last:
                settle(h, total)
            else:
                mix[h] = total

        for g in range(0, heads, group):
            for stage in (score, soften, gather):
                for h in range(g, g + group):
                    stage(h)

    attend_own()
    kv_ring(late, 1)

    def ring_step(t, _):
        @pl.when(t > 1)
        def _():
            kv_ring(late, t)

        def half_step(other, _):
            @pl.when((other == 0) & (t == far))
            def _():
                wo_cross(far)
                wo_fourth(far - 1)

            @pl.when(other == 1)
            def _():
                @pl.when(t < far)
                def _():
                    wo_ring(t + 1)

                @pl.when((t > 0) & (t < far))
                def _():
                    kv_ring(early, t + 1)
                    wo_cross(t)

                @pl.when((t > 1) & (t < far))
                def _():
                    wo_fourth(t - 1)

                pl.when(t == far)(lambda: wo_fourth(far))
                kv_mate(t)

            ln = lane + other * (1 - 2 * lane)
            below, above = z - t, z + t - ring
            middle = (t > 0) & (t < far)
            two = middle & (above >= 0)
            one = (middle & (below >= 0) & (above < 0)) | ((t == 0) & (other == 1) & (lane == 1)) | ((t == far) & (other == 0) & (below >= 0))
            pl.when(two)(lambda: attend([2 * below + ln, 2 * above + ln]))
            pl.when(one)(lambda: attend([2 * below + ln]))

        lax.fori_loop(0, 2, half_step, None)

    lax.fori_loop(0, far + 1, ring_step, None)

    pl.when(z >= far)(lambda: attend([2 * (z - far) + 1 - lane], last=True))

    @pl.when(z < far)
    def _():
        for h in range(heads):
            settle(h, mix[h])

    arrive(wo.at[pl.ds(0, nd // 2 * rows), :], do)
    n_out = depth // wide

    def out_copy(n):
        at = pl.ds(pl.multiple_of(n * wide, wide), wide)
        return pltpu.make_async_copy(a.at[:, at], y_hbm.at[:, at], out_sem.at[n])

    def finish(n, _):
        at = pl.ds(pl.multiple_of(n * wide, wide), wide)
        a[:, at] = (xs[:, at].astype(F32) + _dot(seen[...], wo[:, at])).astype(BF16)
        out_copy(n).start()

    lax.fori_loop(0, n_out, finish, None)
    drain(wkv, skv)
    drain(wq, sq)
    drain(wo, so)
    remote(kall.at[pl.ds(0, 2 * (2 * far - 1))], sk, sk, mate).wait_send()
    remote(kall, sd, sd, mate).wait_send()
    for n in range(n_out):
        out_copy(n).wait()


def _hand_on(src, dst, buf, into, out):
    strips = into.shape[0]
    size = src.shape[0] // strips
    reads, writes = [], []
    for i in range(strips):
        at = pl.ds(i * size, size)
        reads.append(pltpu.make_async_copy(src.at[at, :], buf.at[at, :], into.at[i]))
        writes.append(pltpu.make_async_copy(buf.at[at, :], dst.at[at, :], out.at[i]))
    for read in reads:
        read.start()
    for read, write in zip(reads, writes):
        read.wait()
        write.start()
    for write in writes:
        write.wait()


def solution(mesh):
    side = math.isqrt(mesh.shape["dp"])
    nd = mesh.shape["sp"]
    steps = nd // 4

    def step(x, gain, wq, wk, wv, wo):
        own, depth = x.shape
        heads = wq.shape[1] // HEAD
        anywhere = pl.BlockSpec(memory_space=pl.ANY)
        vmem = pl.BlockSpec(memory_space=pltpu.VMEM)
        dma = pltpu.SemaphoreType.DMA
        flops = 2 * own * depth * (heads + 2) * HEAD + 2 * own * heads * HEAD * depth + 4 * own * own * nd * heads * HEAD // 2
        ring = dma((2, 2, steps))
        y = pl.pallas_call(
            functools.partial(_kernel, side),
            out_shape=jax.ShapeDtypeStruct(x.shape, x.dtype),
            in_specs=[anywhere, vmem, anywhere, anywhere, anywhere, anywhere],
            out_specs=anywhere,
            scratch_shapes=[
                pltpu.VMEM((depth, 2 * HEAD), BF16),
                pltpu.VMEM((depth, heads * HEAD), BF16),
                pltpu.VMEM((heads * HEAD, depth), BF16),
                pltpu.VMEM((nd, own, HEAD), BF16),
                pltpu.VMEM((nd, HEAD, own), BF16),
                pltpu.VMEM((own, depth), BF16),
                pltpu.VMEM((own, depth), BF16),
                pltpu.VMEM((own, heads * HEAD), F32),
                pltpu.VMEM((heads, HEAD, own), BF16),
                pltpu.VMEM((heads, HEAD + 8, own), F32),
                pltpu.VMEM((heads, own), F32),
                pltpu.VMEM((own, heads * HEAD), BF16),
                pltpu.VMEM((own, HEAD // 2), F32),
                pltpu.VMEM((own, HEAD // 2), F32),
                dma((4,)),
                ring, dma((steps,)), dma, dma,
                ring, dma((steps,)), dma((steps + 1,)), dma,
                dma((steps,)), dma((steps,)), dma((steps,)), dma, dma,
                ring, dma((steps + 1,)), dma, dma,
                dma((depth // 512,)),
            ],
            compiler_params=pltpu.CompilerParams(collective_id=0, has_side_effects=True, vmem_limit_bytes=VMEM_LIMIT),
            cost_estimate=pl.CostEstimate(flops=flops, bytes_accessed=4 * x.size * 2, transcendentals=own * own * nd * heads // 2),
        )(x, gain, wq, wk, wv, wo)
        return pl.pallas_call(
            _hand_on,
            out_shape=jax.ShapeDtypeStruct(x.shape, x.dtype),
            in_specs=[anywhere],
            out_specs=anywhere,
            scratch_shapes=[pltpu.VMEM(x.shape, x.dtype), dma((8,)), dma((8,))],
            compiler_params=pltpu.CompilerParams(vmem_limit_bytes=VMEM_LIMIT),
            cost_estimate=pl.CostEstimate(flops=0, bytes_accessed=4 * x.size, transcendentals=0),
        )(y)

    tokens, whole = P(("dp", "sp"), None), P("sp", None)
    return jax.shard_map(
        step,
        mesh=mesh,
        in_specs=(tokens, P(None), whole, whole, whole, whole),
        out_specs=tokens,
        check_vma=False,
    )
```
